16 devices in a mesh: data: 4 (over z, y), expert: 4 (over x, core).
Axes of the slice: x: 2, y: 2, z: 2, core: 2. Of those that a mesh axis runs over, the one named last changes fastest.
Arguments:
- x: bfloat16 [8192, 4096], P(('data', 'expert')), parts along dimension 0
- idx: int32 [8192, 2], P(('data', 'expert')), parts along dimension 0
- wr: bfloat16 [4096, 4], replicated
- w1: bfloat16 [4, 4096, 14336], P('expert')
- w3: bfloat16 [4, 4096, 14336], P('expert')
- w2: bfloat16 [4, 14336, 4096], P('expert')
Outputs:
- output: bfloat16 [8192, 4096], P(('data', 'expert')), parts along dimension 0
There are 4 independent parts. The reference program is written for one: setup_inputs(seed, part) draws one part's arguments, and reference() takes and returns one part's arrays. A program takes and returns all parts, laid end to end along the dimension named above; an argument that names none is the same for every part.
All inputs are finite; a program needn't handle non-finite values.
Results may differ from the reference program's by a relative error of at most 0.001.
Values are sent between devices in bfloat16 or wider.
A program may use at most 1.5 GiB of HBM per device.

```python
import jax
import jax.numpy as jnp
from jax import lax

N = 4
T = 512
D = 4096
FF = 14336
TOP = 2
E = 4
CS = 512


def _routing(key):
    h = E // 2

    def one(k):
        kh, kp, ks = jax.random.split(k, 3)
        hot = jax.random.permutation(kh, E)[:h]
        p = jax.random.permutation(kp, T)
        e0 = hot[p % h]
        e1 = (e0 + 1 + (p // h) % (E - 1)) % E
        pair = jnp.stack([e0, e1], axis=1)
        swap = jax.random.bernoulli(ks, 0.5, (T, 1))
        return jnp.where(swap, pair[:, ::-1], pair)
    return jax.vmap(one)(jax.random.split(key, N)).reshape(N * T, TOP).astype(jnp.int32)


def setup_inputs(seed: int = 0, part: int = 0) -> dict:
    key = jax.random.key(seed)
    kshared, kpart = jax.random.split(key)
    kx, ki = jax.random.split(jax.random.fold_in(kpart, part))
    kr, k1, k3, k2 = jax.random.split(kshared, 4)
    x = jax.random.normal(kx, (N * T, D), jnp.float32).astype(jnp.bfloat16)
    wr = (jax.random.normal(kr, (D, E), jnp.float32) * (1.5 * D ** -0.5)).astype(jnp.bfloat16)
    w1 = (jax.random.normal(k1, (E, D, FF), jnp.float32) * D ** -0.5).astype(jnp.bfloat16)
    w3 = (jax.random.normal(k3, (E, D, FF), jnp.float32) * D ** -0.5).astype(jnp.bfloat16)
    w2 = (jax.random.normal(k2, (E, FF, D), jnp.float32) * FF ** -0.5).astype(jnp.bfloat16)
    return {'x': x, 'idx': _routing(jax.random.fold_in(ki, 7)), 'wr': wr, 'w1': w1, 'w3': w3, 'w2': w2}


def reference(x, idx, wr, w1, w3, w2):
    logits = jnp.dot(x, wr, preferred_element_type=jnp.float32)
    g = jax.nn.softmax(jnp.take_along_axis(logits, idx, axis=1), axis=-1)
    e = idx.reshape(N, T * TOP)
    oh = (e[:, :, None] == jnp.arange(E, dtype=jnp.int32)[None, None, :]).astype(jnp.int32)
    pos = jnp.take_along_axis(jnp.cumsum(oh, axis=1), e[:, :, None], axis=2)[:, :, 0] - 1
    src = jnp.arange(N, dtype=jnp.int32)[:, None]
    valid = (pos < CS).reshape(-1)
    dest = jnp.where(valid, ((e * N + src) * CS + pos).reshape(-1), E * N * CS)
    rows = jnp.repeat(x, TOP, axis=0)
    buf = jnp.zeros((E * N * CS, D), jnp.bfloat16).at[dest].set(rows, mode='drop').reshape(E, N * CS, D)

    def expert(args):
        xb, a1, a3, a2 = args
        h1 = jnp.dot(xb, a1, preferred_element_type=jnp.float32)
        h3 = jnp.dot(xb, a3, preferred_element_type=jnp.float32)
        h = (jax.nn.silu(h1) * h3).astype(jnp.bfloat16)
        return jnp.dot(h, a2, preferred_element_type=jnp.float32).astype(jnp.bfloat16)

    o = lax.map(expert, (buf, w1, w3, w2)).reshape(E * N * CS, D)
    op = jnp.where(valid[:, None], o[jnp.where(valid, dest, 0)], 0)
    y = jnp.sum(g[:, :, None] * op.reshape(N * T, TOP, D).astype(jnp.float32), axis=1)
    return y.astype(jnp.bfloat16)
```

```python
import functools
import jax, jax.numpy as jnp
from jax import lax
from jax.experimental import pallas as pl
from jax.experimental.pallas import tpu as pltpu
from jax.sharding import PartitionSpec as P

RB = 32
NS = 8
CH = 8


def mlp_kernel(axis, big, small, idx_ref, x_hbm, w1, w3, w2, o_hbm, xs, oh, xg, h, ob, wa, wb, sa, sb, sx, so):
    kd = xg.shape[0]
    kf = h.shape[0]
    nn = ob.shape[1] // 512
    t = xs.shape[0]
    ts = t // 256
    c1 = kf * kd // CH
    cpf = kd // CH
    cpn = kf // CH
    total = c1 + nn * cpn
    rows = big * RB

    def src1(w, c):
        f, q = c // cpf, lax.rem(c, cpf)
        return w.at[pl.ds(pl.multiple_of(q * (CH * 256), CH * 256), CH * 256), pl.ds(pl.multiple_of(f * 256, 256), 256)]

    def src2(c, half):
        d = c - c1
        j, q = d // cpn, lax.rem(d, cpn)
        return w2.at[pl.ds(pl.multiple_of(q * (CH * 256), CH * 256), CH * 256), pl.ds(pl.multiple_of(j * 512 + half * 256, 256), 256)]

    def start1(c, s):
        pltpu.make_async_copy(src1(w1, c), wa.at[s], sa.at[s]).start(priority=1)
        pltpu.make_async_copy(src1(w3, c), wb.at[s], sb.at[s]).start(priority=1)

    def start2(c, s):
        pltpu.make_async_copy(src2(c, 0), wa.at[s], sa.at[s]).start(priority=1)
        pltpu.make_async_copy(src2(c, 1), wb.at[s], sb.at[s]).start(priority=1)

    def wait(s):
        pltpu.make_async_copy(w1.at[pl.ds(0, CH * 256), pl.ds(0, 256)], wa.at[s], sa.at[s]).wait()
        pltpu.make_async_copy(w1.at[pl.ds(0, CH * 256), pl.ds(0, 256)], wb.at[s], sb.at[s]).wait()

    def xpiece(j):
        cols = pl.ds(pl.multiple_of(j * 512, 512), 512)
        return pltpu.make_async_copy(x_hbm.at[:, cols], xs.at[:, cols], sx.at[j])

    for j in range(nn):
        xpiece(j).start()
    for c in range(NS - 1):
        start1(c, c)

    e = lax.axis_index(axis)
    has = jnp.where((idx_ref[0:1, :] == e) | (idx_ref[1:2, :] == e), 1.0, 0.0)
    lane = lax.broadcasted_iota(jnp.int32, (1, t), 1)
    cnt = has
    sh = 1
    while sh < t:
        cnt = cnt + jnp.where(lane >= sh, pltpu.roll(cnt, sh, 1), 0.0)
        sh *= 2
    dest = jnp.where(has > 0.0, cnt.astype(jnp.int32) - 1, -1)
    n = jnp.max(cnt).astype(jnp.int32)

    def push(s, u):
        pltpu.matmul_push_rhs(wa[s, u * 256:(u + 1) * 256, :], 0, 0)
        pltpu.matmul_push_rhs(wb[s, u * 256:(u + 1) * 256, :], 0, 1)

    def run(accs, base, more, R):
        def accumulate(par, lhs):
            for r in range(R):
                v = lhs(r)
                pltpu.matmul_acc_lhs(accs[par][0][r], v, load_staged_rhs=0 if r == 0 else None)
                pltpu.matmul_acc_lhs(accs[par][1][r], v, load_staged_rhs=0 if r == 0 else None)

        def sl(r):
            return slice(r * RB, (r + 1) * RB)

        def block(c, lhs, par, stage2, pop):
            s, ns, ps = lax.rem(c, NS), lax.rem(c + 1, NS), lax.rem(c + NS - 1, NS)
            nc = c + NS - 1
            if not stage2:
                pl.when(nc < c1)(lambda: start1(nc, ps))
                pl.when(nc >= c1)(lambda: start2(nc, ps))
            else:
                pl.when(nc < total)(lambda: start2(nc, ps))
                pl.when(more & (nc >= total))(lambda: start1(nc - total, ps))
            for u in range(CH):
                if u == CH - 1:
                    if stage2:
                        pl.when(c + 1 < total)(lambda: wait(ns))
                    else:
                        wait(ns)
                accumulate(par, lambda r: lhs(u, r))
                if u < CH - 1:
                    push(s, u + 1)
                else:
                    push(jnp.where(c + 1 < total, ns, s) if stage2 else ns, 0)
                if u == 0 and pop is not None:
                    pop()

        def pop1(par, f):
            for r in range(R):
                a = pltpu.matmul_pop(accs[par][0][r])
                b = pltpu.matmul_pop(accs[par][1][r])
                h[f, sl(r), :] = (a / (1.0 + jnp.exp(-a)) * b).astype(jnp.bfloat16)

        full = base + R * RB <= t
        tail = t % rows

        def put(j, op):
            cols = pl.ds(pl.multiple_of(j * 512, 512), 512)

            def go(m):
                cp = pltpu.make_async_copy(ob.at[pl.ds(0, m), cols], o_hbm.at[pl.ds(pl.multiple_of(base, RB), m), cols], so.at[j])
                getattr(cp, op)()
            if tail and tail < R * RB:
                pl.when(full)(lambda: go(R * RB))
                pl.when(jnp.logical_not(full))(lambda: go(tail))
            else:
                go(R * RB)

        def pop2(par, j):
            for r in range(R):
                a = pltpu.matmul_pop(accs[par][0][r])
                b = pltpu.matmul_pop(accs[par][1][r])
                c0 = pl.multiple_of(j * 512, 512)
                ob[sl(r), pl.ds(c0, 256)] = a.astype(jnp.bfloat16)
                ob[sl(r), pl.ds(pl.multiple_of(c0 + 256, 256), 256)] = b.astype(jnp.bfloat16)

        iota = lax.broadcasted_iota(jnp.int32, (RB, 256), 0)
        for k in range(ts):
            for r in range(R):
                hit = iota + (base + r * RB) == dest[0:1, k * 256:(k + 1) * 256]
                oh[k, sl(r), :] = jnp.where(hit, 1.0, 0.0).astype(jnp.bfloat16)

        def xpush(j, k):
            c0 = pl.multiple_of(j * 512, 512)
            pltpu.matmul_push_rhs(xs[k * 256:(k + 1) * 256, pl.ds(c0, 256)], 0, 0)
            pltpu.matmul_push_rhs(xs[k * 256:(k + 1) * 256, pl.ds(pl.multiple_of(c0 + 256, 256), 256)], 0, 1)

        def popx(par, j):
            for r in range(R):
                xg[2 * j, sl(r), :] = pltpu.matmul_pop(accs[par][0][r]).astype(jnp.bfloat16)
                xg[2 * j + 1, sl(r), :] = pltpu.matmul_pop(accs[par][1][r]).astype(jnp.bfloat16)

        pl.when(base == 0)(lambda: xpiece(0).wait())
        xpush(0, 0)

        def gat(i, carry):
            for par in range(2):
                j = 2 * i + par
                for k in range(ts):
                    if k == ts - 1:
                        pl.when((base == 0) & (j + 1 < nn))(lambda: xpiece(j + 1).wait())
                    accumulate(par, lambda r: oh[k, sl(r), :])
                    if k < ts - 1:
                        xpush(j, k + 1)
                    else:
                        xpush(lax.rem(j + 1, nn), 0)
                    if k == 0:
                        popx(1 - par, lax.rem(j + nn - 1, nn))
            return carry
        lax.fori_loop(0, nn // 2, gat, 0)
        wait(0)
        z = jnp.zeros((RB, 256), jnp.bfloat16)
        pltpu.matmul_acc_lhs(accs[0][0][0], z, load_staged_rhs=0)
        pltpu.matmul_acc_lhs(accs[0][1][0], z, load_staged_rhs=0)
        push(0, 0)
        popx(1, nn - 1)

        def stage1(i, carry):
            for par in range(2):
                f = 2 * i + par
                for q in range(cpf):
                    block(f * cpf + q, lambda u, r: xg[q * CH + u, sl(r), :], par, False,
                          functools.partial(pop1, 1 - par, lax.rem(f + kf - 1, kf)) if q == 0 else None)
            return carry
        lax.fori_loop(0, kf // 2, stage1, 0)
        pop1(1, kf - 1)

        def stage2(i, carry):
            for par in range(2):
                j = 2 * i + par
                c0 = c1 + j * cpn
                jp = lax.rem(j + nn - 1, nn)

                def go(q, pop):
                    block(c0 + q, lambda u, r: h[q * CH + u, sl(r), :], par, True, pop)

                def out():
                    pop2(1 - par, jp)
                go(0, out)
                if par == 0:
                    pl.when(i > 0)(lambda: put(jp, "start"))
                else:
                    put(jp, "start")

                def inner(q, carry):
                    go(q, None)
                    return carry
                lax.fori_loop(1, cpn, inner, 0)
            return carry
        lax.fori_loop(0, nn // 2, stage2, 0)
        pltpu.matmul_acc_lhs(accs[0][0][0], z, load_staged_rhs=0)
        pltpu.matmul_acc_lhs(accs[0][1][0], z, load_staged_rhs=0)
        pop2(1, nn - 1)
        put(nn - 1, "start")
        pltpu.matmul_pop(accs[0][0][0])
        pltpu.matmul_pop(accs[0][1][0])
        for j in range(nn):
            put(j, "wait")

    def scoped(*refs):
        it = iter(refs)
        accs = [[[next(it) for _ in range(big)] for _ in range(2)] for _ in range(2)]

        def tile(s, carry):
            base = s * rows
            more = n > base + rows
            lax.cond(n - base <= small * RB, lambda: run(accs, base, more, small), lambda: run(accs, base, more, big))
            return carry
        lax.fori_loop(0, (n + rows - 1) // rows, tile, 0)

        @pl.when(n == 0)
        def _():
            for j in range(nn):
                xpiece(j).wait()
            for s in range(NS - 1):
                wait(s)

    pl.run_scoped(scoped, *[pltpu.ACC(q)((RB, 256), jnp.float32) for _ in range(2) for q in range(2) for _ in range(big)])


def mlp(axis, idx, x, w1, w3, w2, big=11, small=6):
    t, d = x.shape
    ff = w1.shape[1]
    return pl.pallas_call(
        functools.partial(mlp_kernel, axis, big, small),
        out_shape=jax.ShapeDtypeStruct((t, d), jnp.bfloat16),
        in_specs=[pl.BlockSpec(memory_space=pltpu.VMEM)] + [pl.BlockSpec(memory_space=pl.ANY)] * 4,
        out_specs=pl.BlockSpec(memory_space=pl.ANY),
        scratch_shapes=[
            pltpu.VMEM((t, d), jnp.bfloat16),
            pltpu.VMEM((t // 256, big * RB, 256), jnp.bfloat16),
            pltpu.VMEM((d // 256, big * RB, 256), jnp.bfloat16),
            pltpu.VMEM((ff // 256, big * RB, 256), jnp.bfloat16),
            pltpu.VMEM((big * RB, d), jnp.bfloat16),
            pltpu.VMEM((NS, CH * 256, 256), jnp.bfloat16),
            pltpu.VMEM((NS, CH * 256, 256), jnp.bfloat16),
            pltpu.SemaphoreType.DMA((NS,)),
            pltpu.SemaphoreType.DMA((NS,)),
            pltpu.SemaphoreType.DMA((d // 512,)),
            pltpu.SemaphoreType.DMA((d // 512,)),
        ],
        compiler_params=pltpu.CompilerParams(vmem_limit_bytes=60 * 1024 * 1024),
        cost_estimate=pl.CostEstimate(flops=6 * big * RB * d * ff, bytes_accessed=6 * d * ff, transcendentals=0),
        name="expert_rows",
    )(idx, x, w1, w3, w2)


def prep_kernel(axis, n, x_ref, wr_ref, idx_ref, g_ref, d_ref, c_ref):
    t = x_ref.shape[0]
    me = lax.axis_index(axis)
    logits = jnp.dot(x_ref[...], wr_ref[...], preferred_element_type=jnp.float32)
    i0, i1 = idx_ref[:, 0:1], idx_ref[:, 1:2]
    s0 = jnp.zeros((t, 1), jnp.float32)
    s1 = jnp.zeros((t, 1), jnp.float32)
    for e in range(n):
        s0 = s0 + jnp.where(i0 == e, logits[:, e:e + 1], 0.0)
        s1 = s1 + jnp.where(i1 == e, logits[:, e:e + 1], 0.0)
    m = jnp.maximum(s0, s1)
    p0, p1 = jnp.exp(s0 - m), jnp.exp(s1 - m)
    g0, g1 = p0 / (p0 + p1), p1 / (p0 + p1)
    slot = lax.broadcasted_iota(jnp.int32, (1, n), 1)
    e = me ^ slot
    h0, h1 = jnp.where(i0 == e, 1.0, 0.0), jnp.where(i1 == e, 1.0, 0.0)
    g_ref[...] = h0 * g0 + h1 * g1
    has = h0 + h1
    tri = lax.broadcasted_iota(jnp.int32, (t, t), 0) >= lax.broadcasted_iota(jnp.int32, (t, t), 1)
    tri = jnp.where(tri, 1.0, 0.0).astype(jnp.bfloat16)
    cnt = jnp.dot(tri, has.astype(jnp.bfloat16), preferred_element_type=jnp.float32)
    d_ref[...] = jnp.where(has > 0.0, cnt.astype(jnp.int32) - 1, -1)
    c_ref[...] = jnp.max(cnt, axis=0, keepdims=True).astype(jnp.int32)


def prep(axis, n, x, wr, idx):
    t, d = x.shape
    vm = pl.BlockSpec(memory_space=pltpu.VMEM)
    return pl.pallas_call(
        functools.partial(prep_kernel, axis, n),
        out_shape=(jax.ShapeDtypeStruct((t, n), jnp.float32), jax.ShapeDtypeStruct((t, n), jnp.int32), jax.ShapeDtypeStruct((1, n), jnp.int32)),
        in_specs=[vm] * 3,
        out_specs=(vm,) * 3,
        cost_estimate=pl.CostEstimate(flops=2 * t * d * 128, bytes_accessed=t * d * 2, transcendentals=0),
        name="gates",
    )(x, wr, idx)


def combine_kernel(d_ref, g_ref, n_ref, *refs):
    k = len(refs) - 2
    o_refs, y_ref, sel = refs[:k], refs[k], refs[k + 1]
    t = y_ref.shape[0]
    rows = o_refs[0].shape[0]

    @pl.when(pl.program_id(0) == 0)
    def _():
        iota = lax.broadcasted_iota(jnp.int32, (t, rows), 1)
        for e in range(k):
            sel[e] = jnp.where(iota == d_ref[:, e:e + 1], 1.0, 0.0).astype(jnp.bfloat16)

    rid = lax.broadcasted_iota(jnp.int32, (rows, y_ref.shape[1]), 0)
    y = None
    for e in range(k):
        o = o_refs[e][...]
        o = jnp.where(rid < n_ref[0:1, e:e + 1], o, jnp.zeros_like(o))
        p = g_ref[:, e:e + 1] * jnp.dot(sel[e], o, preferred_element_type=jnp.float32)
        y = p if y is None else y + p
    y_ref[...] = y.astype(y_ref.dtype)


def combine(d, g, n, outs, cols=512):
    t, width = outs[0].shape
    k = len(outs)
    whole = lambda i: (0, 0)
    return pl.pallas_call(
        combine_kernel,
        grid=(width // cols,),
        out_shape=jax.ShapeDtypeStruct((t, width), jnp.bfloat16),
        in_specs=[pl.BlockSpec((t, k), whole), pl.BlockSpec((t, k), whole), pl.BlockSpec((1, k), whole)]
        + [pl.BlockSpec((t, cols), lambda i: (0, i))] * k,
        out_specs=pl.BlockSpec((t, cols), lambda i: (0, i)),
        scratch_shapes=[pltpu.VMEM((k, t, t), jnp.bfloat16)],
        cost_estimate=pl.CostEstimate(flops=2 * k * t * t * width, bytes_accessed=(k + 1) * t * width * 2, transcendentals=0),
        name="combine_rows",
    )(d, g, n, *outs)


def solution(mesh):
    n = mesh.shape['expert']

    def hop(a, bit):
        return lax.ppermute(a, 'expert', [(i, i ^ bit) for i in range(n)])

    def local(x, idx, wr, w1, w3, w2):
        w1, w3, w2 = w1[0], w3[0], w2[0]
        idx_1, x_1 = hop(idx, 1), hop(x, 1)
        idx_2, x_2 = hop(idx, 2), hop(x, 2)
        idx_3, x_3 = hop(idx_2, 1), hop(x_2, 1)
        g, d, c = prep('expert', n, x, wr, idx)
        outs, tie = {}, None
        for b, (xi, ii) in {1: (x_1, idx_1), 2: (x_2, idx_2), 3: (x_3, idx_3), 0: (x, idx)}.items():
            if tie is not None:
                ii, outs[tie] = lax.optimization_barrier((ii, outs[tie]))
            outs[b] = mlp('expert', ii.T, xi, w1, w3, w2)
            tie = b
        back = [outs[0]] + [hop(outs[b], b) for b in (1, 2, 3)]
        return combine(d, g, c, back)

    tok = P(('data', 'expert'), None)
    wsp = P('expert', None, None)
    return jax.shard_map(local, mesh=mesh, in_specs=(tok, tok, P(), wsp, wsp, wsp), out_specs=tok, check_vma=False)
```

```python
import functools
import jax, jax.numpy as jnp
from jax import lax
from jax.experimental import pallas as pl
from jax.experimental.pallas import tpu as pltpu
from jax.sharding import PartitionSpec as P

RB = 32
NS = 8
CH = 8


def mlp_kernel(axis, big, small, resident, idx_ref, x_ref, w1, w3, w2, o_ref, oh, xg, h, wa, wb, sa, sb, *rest):
    if resident:
        xs, ob = x_ref, o_ref
    else:
        xs, ob, zs, sx, so, sz = rest
    kd = xg.shape[0]
    kf = h.shape[0]
    nn = o_ref.shape[1] // 512
    t = x_ref.shape[0]
    ts = t // 256
    c1 = kf * kd // CH
    cpf = kd // CH
    cpn = kf // CH
    total = c1 + nn * cpn
    rows = big * RB

    def src1(w, c):
        f, q = c // cpf, lax.rem(c, cpf)
        return w.at[pl.ds(pl.multiple_of(q * (CH * 256), CH * 256), CH * 256), pl.ds(pl.multiple_of(f * 256, 256), 256)]

    def src2(c, half):
        d = c - c1
        j, q = d // cpn, lax.rem(d, cpn)
        return w2.at[pl.ds(pl.multiple_of(q * (CH * 256), CH * 256), CH * 256), pl.ds(pl.multiple_of(j * 512 + half * 256, 256), 256)]

    def start1(c, s):
        pltpu.make_async_copy(src1(w1, c), wa.at[s], sa.at[s]).start(priority=1)
        pltpu.make_async_copy(src1(w3, c), wb.at[s], sb.at[s]).start(priority=1)

    def start2(c, s):
        pltpu.make_async_copy(src2(c, 0), wa.at[s], sa.at[s]).start(priority=1)
        pltpu.make_async_copy(src2(c, 1), wb.at[s], sb.at[s]).start(priority=1)

    def wait(s):
        pltpu.make_async_copy(w1.at[pl.ds(0, CH * 256), pl.ds(0, 256)], wa.at[s], sa.at[s]).wait()
        pltpu.make_async_copy(w1.at[pl.ds(0, CH * 256), pl.ds(0, 256)], wb.at[s], sb.at[s]).wait()

    def xpiece(j):
        cols = pl.ds(pl.multiple_of(j * 512, 512), 512)
        return pltpu.make_async_copy(x_ref.at[:, cols], xs.at[:, cols], sx.at[j])

    if not resident:
        for j in range(nn):
            xpiece(j).start()
    for c in range(NS - 1):
        start1(c, c)

    e = lax.axis_index(axis)
    has = jnp.where((idx_ref[0:1, :] == e) | (idx_ref[1:2, :] == e), 1.0, 0.0)
    lane = lax.broadcasted_iota(jnp.int32, (1, t), 1)
    cnt = has
    sh = 1
    while sh < t:
        cnt = cnt + jnp.where(lane >= sh, pltpu.roll(cnt, sh, 1), 0.0)
        sh *= 2
    dest = jnp.where(has > 0.0, cnt.astype(jnp.int32) - 1, -1)
    n = jnp.max(cnt).astype(jnp.int32)

    z = jnp.zeros((RB, 256), jnp.bfloat16)
    if not resident:
        spare = pltpu.make_async_copy(zs, o_ref.at[pl.ds(rows, t - rows)], sz)

        @pl.when(n <= rows)
        def _():
            zs[...] = jnp.zeros_like(zs)
            spare.start()

    def push(s, u):
        pltpu.matmul_push_rhs(wa[s, u * 256:(u + 1) * 256, :], 0, 0)
        pltpu.matmul_push_rhs(wb[s, u * 256:(u + 1) * 256, :], 0, 1)

    def run(accs, base, more, R):
        def accumulate(par, lhs):
            for r in range(R):
                v = lhs(r)
                pltpu.matmul_acc_lhs(accs[par][0][r], v, load_staged_rhs=0 if r == 0 else None)
                pltpu.matmul_acc_lhs(accs[par][1][r], v, load_staged_rhs=0 if r == 0 else None)

        def sl(r):
            return slice(r * RB, (r + 1) * RB)

        def block(c, lhs, par, stage2, pop):
            s, ns, ps = lax.rem(c, NS), lax.rem(c + 1, NS), lax.rem(c + NS - 1, NS)
            nc = c + NS - 1
            if not stage2:
                pl.when(nc < c1)(lambda: start1(nc, ps))
                pl.when(nc >= c1)(lambda: start2(nc, ps))
            else:
                pl.when(nc < total)(lambda: start2(nc, ps))
                pl.when(more & (nc >= total))(lambda: start1(nc - total, ps))
            for u in range(CH):
                if u == CH - 1:
                    if stage2:
                        pl.when(c + 1 < total)(lambda: wait(ns))
                    else:
                        wait(ns)
                accumulate(par, lambda r: lhs(u, r))
                if u < CH - 1:
                    push(s, u + 1)
                else:
                    push(jnp.where(c + 1 < total, ns, s) if stage2 else ns, 0)
                if u == 0 and pop is not None:
                    pop()

        def pop1(par, f):
            for r in range(R):
                a = pltpu.matmul_pop(accs[par][0][r])
                b = pltpu.matmul_pop(accs[par][1][r])
                h[f, sl(r), :] = (a / (1.0 + jnp.exp(-a)) * b).astype(jnp.bfloat16)

        def put(j, op):
            cols = pl.ds(pl.multiple_of(j * 512, 512), 512)

            def go(first, m):
                cp = pltpu.make_async_copy(ob.at[pl.ds(0, m), cols], o_ref.at[pl.ds(first, m), cols], so.at[j])
                getattr(cp, op)()
            pl.when(base == 0)(lambda: go(0, rows))
            pl.when(base > 0)(lambda: go(rows, t - rows))

        def pop2(par, j):
            c0 = pl.multiple_of(j * 512, 512)
            for r in range(big):
                first = pl.multiple_of((base if resident else 0) + r * RB, RB)
                if r < R:
                    a = pltpu.matmul_pop(accs[par][0][r]).astype(jnp.bfloat16)
                    b = pltpu.matmul_pop(accs[par][1][r]).astype(jnp.bfloat16)
                else:
                    a = b = z

                def store(first=first, a=a, b=b):
                    ob[pl.ds(first, RB), pl.ds(c0, 256)] = a
                    ob[pl.ds(first, RB), pl.ds(pl.multiple_of(c0 + 256, 256), 256)] = b
                if resident and R == small and rows + r * RB >= t:
                    pl.when(first < t)(store)
                else:
                    store()

        iota = lax.broadcasted_iota(jnp.int32, (RB, 256), 0)
        for k in range(ts):
            for r in range(R):
                hit = iota + (base + r * RB) == dest[0:1, k * 256:(k + 1) * 256]
                oh[k, sl(r), :] = jnp.where(hit, 1.0, 0.0).astype(jnp.bfloat16)

        def xpush(j, k):
            c0 = pl.multiple_of(j * 512, 512)
            pltpu.matmul_push_rhs(xs[k * 256:(k + 1) * 256, pl.ds(c0, 256)], 0, 0)
            pltpu.matmul_push_rhs(xs[k * 256:(k + 1) * 256, pl.ds(pl.multiple_of(c0 + 256, 256), 256)], 0, 1)

        def popx(par, j):
            for r in range(R):
                xg[2 * j, sl(r), :] = pltpu.matmul_pop(accs[par][0][r]).astype(jnp.bfloat16)
                xg[2 * j + 1, sl(r), :] = pltpu.matmul_pop(accs[par][1][r]).astype(jnp.bfloat16)

        if not resident:
            pl.when(base == 0)(lambda: xpiece(0).wait())
        xpush(0, 0)

        def gat(i, carry):
            for par in range(2):
                j = 2 * i + par
                for k in range(ts):
                    if k == ts - 1 and not resident:
                        pl.when((base == 0) & (j + 1 < nn))(lambda: xpiece(j + 1).wait())
                    accumulate(par, lambda r: oh[k, sl(r), :])
                    if k < ts - 1:
                        xpush(j, k + 1)
                    else:
                        xpush(lax.rem(j + 1, nn), 0)
                    if k == 0:
                        popx(1 - par, lax.rem(j + nn - 1, nn))
            return carry
        lax.fori_loop(0, nn // 2, gat, 0)
        wait(0)
        pltpu.matmul_acc_lhs(accs[0][0][0], z, load_staged_rhs=0)
        pltpu.matmul_acc_lhs(accs[0][1][0], z, load_staged_rhs=0)
        push(0, 0)
        popx(1, nn - 1)

        def stage1(i, carry):
            for par in range(2):
                f = 2 * i + par
                for q in range(cpf):
                    block(f * cpf + q, lambda u, r: xg[q * CH + u, sl(r), :], par, False,
                          functools.partial(pop1, 1 - par, lax.rem(f + kf - 1, kf)) if q == 0 else None)
            return carry
        lax.fori_loop(0, kf // 2, stage1, 0)
        pop1(1, kf - 1)

        def stage2(i, carry):
            for par in range(2):
                j = 2 * i + par
                c0 = c1 + j * cpn
                jp = lax.rem(j + nn - 1, nn)

                def go(q, pop):
                    block(c0 + q, lambda u, r: h[q * CH + u, sl(r), :], par, True, pop)

                def out():
                    pop2(1 - par, jp)
                go(0, out)
                if not resident:
                    if par == 0:
                        pl.when(i > 0)(lambda: put(jp, "start"))
                    else:
                        put(jp, "start")

                def inner(q, carry):
                    go(q, None)
                    return carry
                lax.fori_loop(1, cpn, inner, 0)
            return carry
        lax.fori_loop(0, nn // 2, stage2, 0)
        pltpu.matmul_acc_lhs(accs[0][0][0], z, load_staged_rhs=0)
        pltpu.matmul_acc_lhs(accs[0][1][0], z, load_staged_rhs=0)
        pop2(1, nn - 1)
        if not resident:
            put(nn - 1, "start")
        pltpu.matmul_pop(accs[0][0][0])
        pltpu.matmul_pop(accs[0][1][0])
        if not resident:
            for j in range(nn):
                put(j, "wait")

    def scoped(*refs):
        it = iter(refs)
        accs = [[[next(it) for _ in range(big)] for _ in range(2)] for _ in range(2)]

        def tile(s, carry):
            base = s * rows
            more = n > base + rows
            lax.cond(n - base <= small * RB, lambda: run(accs, base, more, small), lambda: run(accs, base, more, big))
            return carry
        lax.fori_loop(0, jnp.maximum((n + rows - 1) // rows, 1), tile, 0)
        if resident:
            @pl.when(n <= rows)
            def _():
                o_ref[rows:, :] = jnp.zeros((t - rows, o_ref.shape[1]), o_ref.dtype)
        else:
            pl.when(n <= rows)(spare.wait)

    pl.run_scoped(scoped, *[pltpu.ACC(q)((RB, 256), jnp.float32) for _ in range(2) for q in range(2) for _ in range(big)])


def mlp(axis, idx, x, w1, w3, w2, resident, big=11, small=6):
    t, d = x.shape
    ff = w1.shape[1]
    rows = big * RB
    hbm, vmem = pl.BlockSpec(memory_space=pltpu.HBM), pl.BlockSpec(memory_space=pltpu.VMEM)
    io = vmem if resident else hbm
    return pl.pallas_call(
        functools.partial(mlp_kernel, axis, big, small, resident),
        out_shape=jax.ShapeDtypeStruct((t, d), jnp.bfloat16),
        in_specs=[vmem, io, hbm, hbm, hbm],
        out_specs=io,
        scratch_shapes=[
            pltpu.VMEM((t // 256, rows, 256), jnp.bfloat16),
            pltpu.VMEM((d // 256, rows, 256), jnp.bfloat16),
            pltpu.VMEM((ff // 256, rows, 256), jnp.bfloat16),
            pltpu.VMEM((NS, CH * 256, 256), jnp.bfloat16),
            pltpu.VMEM((NS, CH * 256, 256), jnp.bfloat16),
            pltpu.SemaphoreType.DMA((NS,)),
            pltpu.SemaphoreType.DMA((NS,)),
        ]
        + ([] if resident else [
            pltpu.VMEM((t, d), jnp.bfloat16),
            pltpu.VMEM((rows, d), jnp.bfloat16),
            pltpu.VMEM((t - rows, d), jnp.bfloat16),
            pltpu.SemaphoreType.DMA((d // 512,)),
            pltpu.SemaphoreType.DMA((d // 512,)),
            pltpu.SemaphoreType.DMA,
        ]),
        compiler_params=pltpu.CompilerParams(vmem_limit_bytes=41 * 1024 * 1024),
        cost_estimate=pl.CostEstimate(flops=6 * rows * d * ff, bytes_accessed=6 * d * ff, transcendentals=0),
        name="expert_rows",
    )(idx, x, w1, w3, w2)


def prep_kernel(axis, n, x_ref, wr_ref, idx_ref, g_ref, d_ref):
    t = x_ref.shape[0]
    me = lax.axis_index(axis)
    logits = jnp.dot(x_ref[...], wr_ref[...], preferred_element_type=jnp.float32)
    i0, i1 = idx_ref[:, 0:1], idx_ref[:, 1:2]
    s0 = jnp.zeros((t, 1), jnp.float32)
    s1 = jnp.zeros((t, 1), jnp.float32)
    for e in range(n):
        s0 = s0 + jnp.where(i0 == e, logits[:, e:e + 1], 0.0)
        s1 = s1 + jnp.where(i1 == e, logits[:, e:e + 1], 0.0)
    m = jnp.maximum(s0, s1)
    p0, p1 = jnp.exp(s0 - m), jnp.exp(s1 - m)
    g0, g1 = p0 / (p0 + p1), p1 / (p0 + p1)
    slot = lax.broadcasted_iota(jnp.int32, (1, n), 1)
    e = me ^ slot
    h0, h1 = jnp.where(i0 == e, 1.0, 0.0), jnp.where(i1 == e, 1.0, 0.0)
    g_ref[...] = h0 * g0 + h1 * g1
    has = h0 + h1
    tri = lax.broadcasted_iota(jnp.int32, (t, t), 0) >= lax.broadcasted_iota(jnp.int32, (t, t), 1)
    tri = jnp.where(tri, 1.0, 0.0).astype(jnp.bfloat16)
    cnt = jnp.dot(tri, has.astype(jnp.bfloat16), preferred_element_type=jnp.float32)
    d_ref[...] = jnp.where(has > 0.0, cnt.astype(jnp.int32) - 1, -1)


def prep(axis, n, x, wr, idx):
    t, d = x.shape
    vm = pl.BlockSpec(memory_space=pltpu.VMEM)
    return pl.pallas_call(
        functools.partial(prep_kernel, axis, n),
        out_shape=(jax.ShapeDtypeStruct((t, n), jnp.float32), jax.ShapeDtypeStruct((t, n), jnp.int32)),
        in_specs=[vm] * 3,
        out_specs=(vm,) * 2,
        cost_estimate=pl.CostEstimate(flops=2 * t * d * 128, bytes_accessed=t * d * 2, transcendentals=0),
        compiler_params=pltpu.CompilerParams(vmem_limit_bytes=12 * 1024 * 1024),
        name="gates",
    )(x, wr, idx)


def combine_kernel(d_ref, g_ref, o0, o3, h1, h2, y_ref, sel, gb, ya, yt, b1, b2, s1, s2, sy):
    t, width = y_ref.shape
    nn = width // 512
    nr = t // RB
    ts = t // 256

    def cols(j):
        return pl.ds(pl.multiple_of(j * 512, 512), 512)

    def load(j, i):
        h, b, s = ((h1, b1, s1), (h2, b2, s2))[i]
        return pltpu.make_async_copy(h.at[:, cols(j)], b.at[:, cols(j)], s.at[j])

    def out(j):
        return pltpu.make_async_copy(yt.at[lax.rem(j, 2)], y_ref.at[:, cols(j)], sy.at[lax.rem(j, 2)])

    for j in range(nn):
        load(j, 0).start()
        load(j, 1).start()
    order = ((0, o0), (3, o3), (1, b1), (2, b2))
    iota = lax.broadcasted_iota(jnp.int32, (t, t), 1)
    for e in range(len(order)):
        sel[e] = jnp.where(iota == d_ref[:, e:e + 1], 1.0, 0.0).astype(jnp.bfloat16)
        gb[e] = jnp.broadcast_to(g_ref[:, e:e + 1], gb.shape[1:])

    def sl(r):
        return slice(r * RB, (r + 1) * RB)

    def push(o, j, k):
        c0 = pl.multiple_of(j * 512, 512)
        pltpu.matmul_push_rhs(o[k * 256:(k + 1) * 256, pl.ds(c0, 256)], 0, 0)
        pltpu.matmul_push_rhs(o[k * 256:(k + 1) * 256, pl.ds(pl.multiple_of(c0 + 256, 256), 256)], 0, 1)

    def scoped(*refs):
        it = iter(refs)
        accs = [[[next(it) for _ in range(nr)] for _ in range(2)] for _ in range(2)]

        def drain(par, i, slot):
            e = order[i][0]
            for r in range(nr):
                g = gb[e, sl(r), :]
                for q in range(2):
                    p = pltpu.matmul_pop(accs[par][q][r])
                    for c in range(2):
                        at = slice(q * 256 + c * 128, q * 256 + (c + 1) * 128)
                        v = g * p[:, c * 128:(c + 1) * 128]
                        if i > 0:
                            v = ya[sl(r), at] + v
                        if i < len(order) - 1:
                            ya[sl(r), at] = v
                        else:
                            yt[slot, sl(r), at] = v.astype(yt.dtype)

        push(o0, 0, 0)

        def step(j, carry):
            slot = lax.rem(j + 1, 2)
            for i, (e, o) in enumerate(order):
                for k in range(ts):
                    for r in range(nr):
                        v = sel[e, sl(r), k * 256:(k + 1) * 256]
                        for q in range(2):
                            pltpu.matmul_acc_lhs(accs[i % 2][q][r], v, load_staged_rhs=0 if r == 0 else None)
                    if k + 1 < ts:
                        push(o, j, k + 1)
                    elif i + 1 < len(order):
                        if i + 1 >= 2:
                            load(j, i - 1).wait()
                        push(order[i + 1][1], j, 0)
                    else:
                        push(o0, lax.rem(j + 1, nn), 0)
                    if k == 0:
                        if i == 0:
                            pl.when(j > 2)(lambda: out(j - 3).wait())
                            drain(1, len(order) - 1, slot)
                            pl.when(j > 0)(lambda: out(j - 1).start())
                        else:
                            drain((i - 1) % 2, i - 1, slot)
            return carry
        lax.fori_loop(0, nn, step, 0)
        z = jnp.zeros((RB, 256), jnp.bfloat16)
        for q in range(2):
            pltpu.matmul_acc_lhs(accs[0][q][0], z, load_staged_rhs=0)
        out(nn - 3).wait()
        drain(1, len(order) - 1, (nn - 1) % 2)
        out(nn - 1).start()
        for q in range(2):
            pltpu.matmul_pop(accs[0][q][0])
        out(nn - 2).wait()
        out(nn - 1).wait()

    pl.run_scoped(scoped, *[pltpu.ACC(q)((RB, 256), jnp.float32) for _ in range(2) for q in range(2) for _ in range(nr)])


def combine(d, g, outs):
    t, width = outs[0].shape
    k = len(outs)
    hbm, vmem = pl.BlockSpec(memory_space=pltpu.HBM), pl.BlockSpec(memory_space=pltpu.VMEM)
    return pl.pallas_call(
        combine_kernel,
        out_shape=jax.ShapeDtypeStruct((t, width), jnp.bfloat16),
        in_specs=[vmem] * 4 + [hbm] * 2,
        out_specs=hbm,
        scratch_shapes=[
            pltpu.VMEM((k, t, t), jnp.bfloat16),
            pltpu.VMEM((k, t, 128), jnp.float32),
            pltpu.VMEM((t, 512), jnp.float32),
            pltpu.VMEM((2, t, 512), jnp.bfloat16),
            pltpu.VMEM((t, width), jnp.bfloat16),
            pltpu.VMEM((t, width), jnp.bfloat16),
            pltpu.SemaphoreType.DMA((width // 512,)),
            pltpu.SemaphoreType.DMA((width // 512,)),
            pltpu.SemaphoreType.DMA((2,)),
        ],
        compiler_params=pltpu.CompilerParams(vmem_limit_bytes=28 * 1024 * 1024),
        cost_estimate=pl.CostEstimate(flops=2 * k * t * t * width, bytes_accessed=(k + 1) * t * width * 2, transcendentals=0),
        name="combine_rows",
    )(d, g, outs[0], outs[3], outs[1], outs[2])


def solution(mesh):
    n = mesh.shape['expert']

    def hop(a, bit):
        return lax.ppermute(a, 'expert', [(i, i ^ bit) for i in range(n)])

    def local(x, idx, wr, w1, w3, w2):
        w1, w3, w2 = w1[0], w3[0], w2[0]
        idx_1, x_1 = hop(idx, 1), hop(x, 1)
        idx_2, x_2 = hop(idx, 2), hop(x, 2)
        idx_3, x_3 = hop(idx_2, 1), hop(x_2, 1)
        g, d = prep('expert', n, x, wr, idx)
        outs, tie = {}, None
        for b, (xi, ii) in {1: (x_1, idx_1), 2: (x_2, idx_2), 3: (x_3, idx_3), 0: (x, idx)}.items():
            if tie is not None:
                ii, outs[tie] = lax.optimization_barrier((ii, outs[tie]))
            outs[b] = mlp('expert', ii.T, xi, w1, w3, w2, resident=b in (3, 0))
            tie = b
        back = [outs[0]] + [hop(outs[b], b) for b in (1, 2, 3)]
        return combine(d, g, back)

    tok = P(('data', 'expert'), None)
    wsp = P('expert', None, None)
    return jax.shard_map(local, mesh=mesh, in_specs=(tok, tok, P(), wsp, wsp, wsp), out_specs=tok, check_vma=False)
```

```python
import functools
import jax, jax.numpy as jnp
from jax import lax
from jax.experimental import pallas as pl
from jax.experimental.pallas import tpu as pltpu
from jax.sharding import PartitionSpec as P

RB = 32
NS = 8
CH = 8
SUB = 4


def mlp_kernel(axis, big, small, resident, idx_ref, x_ref, w1, w3, w2, o_ref, oh, xg, h, wa, wb, sa, sb, *rest):
    if resident:
        xs, ob = x_ref, o_ref
    else:
        xs, ob, zs, sx, so, sz = rest
    kd = xg.shape[0]
    kf = h.shape[0]
    nn = o_ref.shape[1] // 512
    t = x_ref.shape[0]
    ts = t // 256
    c1 = kf * kd // CH
    cpf = kd // CH
    cpn = kf // CH
    total = c1 + nn * cpn
    rows = big * RB

    def src1(w, c):
        f, q = c // cpf, lax.rem(c, cpf)
        return w.at[pl.ds(pl.multiple_of(q * (CH * 256), CH * 256), CH * 256), pl.ds(pl.multiple_of(f * 256, 256), 256)]

    def src2(c, half):
        d = c - c1
        j, q = d // cpn, lax.rem(d, cpn)
        return w2.at[pl.ds(pl.multiple_of(q * (CH * 256), CH * 256), CH * 256), pl.ds(pl.multiple_of(j * 512 + half * 256, 256), 256)]

    def start1(c, s):
        pltpu.make_async_copy(src1(w1, c), wa.at[s], sa.at[s]).start(priority=1)
        pltpu.make_async_copy(src1(w3, c), wb.at[s], sb.at[s]).start(priority=1)

    def start2(c, s):
        pltpu.make_async_copy(src2(c, 0), wa.at[s], sa.at[s]).start(priority=1)
        pltpu.make_async_copy(src2(c, 1), wb.at[s], sb.at[s]).start(priority=1)

    def wait(s):
        pltpu.make_async_copy(w1.at[pl.ds(0, CH * 256), pl.ds(0, 256)], wa.at[s], sa.at[s]).wait()
        pltpu.make_async_copy(w1.at[pl.ds(0, CH * 256), pl.ds(0, 256)], wb.at[s], sb.at[s]).wait()

    def xpiece(j):
        cols = pl.ds(pl.multiple_of(j * 512, 512), 512)
        return pltpu.make_async_copy(x_ref.at[:, cols], xs.at[:, cols], sx.at[j])

    if not resident:
        for j in range(nn):
            xpiece(j).start()
    for c in range(NS - 1):
        start1(c, c)

    e = lax.axis_index(axis)
    has = jnp.where((idx_ref[0:1, :] == e) | (idx_ref[1:2, :] == e), 1.0, 0.0)
    lane = lax.broadcasted_iota(jnp.int32, (1, t), 1)
    cnt = has
    sh = 1
    while sh < t:
        cnt = cnt + jnp.where(lane >= sh, pltpu.roll(cnt, sh, 1), 0.0)
        sh *= 2
    dest = jnp.where(has > 0.0, cnt.astype(jnp.int32) - 1, -1)
    n = jnp.max(cnt).astype(jnp.int32)

    z = jnp.zeros((RB, 256), jnp.bfloat16)
    if not resident:
        spare = pltpu.make_async_copy(zs, o_ref.at[pl.ds(rows, t - rows)], sz)

        @pl.when(n <= rows)
        def _():
            zs[...] = jnp.zeros_like(zs)
            spare.start()

    def push(s, u):
        pltpu.matmul_push_rhs(wa[s, u * 256:(u + 1) * 256, :], 0, 0)
        pltpu.matmul_push_rhs(wb[s, u * 256:(u + 1) * 256, :], 0, 1)

    def run(accs, base, more, R):
        def accumulate(par, lhs):
            for r in range(R):
                v = lhs(r)
                pltpu.matmul_acc_lhs(accs[par][0][r], v, load_staged_rhs=0 if r == 0 else None)
                pltpu.matmul_acc_lhs(accs[par][1][r], v, load_staged_rhs=0 if r == 0 else None)

        def sl(r):
            return slice(r * RB, (r + 1) * RB)

        def feed(c, ps, stage2):
            nc = c + NS - 1
            if not stage2:
                pl.when(nc < c1)(lambda: start1(nc, ps))
                pl.when(nc >= c1)(lambda: start2(nc, ps))
            else:
                pl.when(nc < total)(lambda: start2(nc, ps))
                pl.when(more & (nc >= total))(lambda: start1(nc - total, ps))

        def block(c, q, src, par, stage2, pop):
            s, ns, ps = lax.rem(c, NS), lax.rem(c + 1, NS), lax.rem(c + NS - 1, NS)
            feed(c, ps, stage2)
            for u in range(CH):
                if u == CH - 1:
                    if stage2:
                        pl.when(c + 1 < total)(lambda: wait(ns))
                    else:
                        wait(ns)
                accumulate(par, lambda r: src[q * CH + u, sl(r), :])
                if u < CH - 1:
                    push(s, u + 1)
                else:
                    push(jnp.where(c + 1 < total, ns, s) if stage2 else ns, 0)
                if u == 0 and pop is not None:
                    pop()

        def rolled(c0, chunks, src, par, stage2, pop):
            def trip(i, carry):
                q, u0 = i // (CH // SUB), lax.rem(i, CH // SUB) * SUB
                c = c0 + q
                s, ns, ps = lax.rem(c, NS), lax.rem(c + 1, NS), lax.rem(c + NS - 1, NS)
                pl.when(u0 == 0)(lambda: feed(c, ps, stage2))
                for u in range(SUB):
                    accumulate(par, lambda r: src[i * SUB + u, sl(r), :])
                    if u < SUB - 1:
                        row, slot = (u0 + u + 1) * 256, s
                    else:
                        ends = u0 + SUB == CH
                        pl.when(ends & (c + 1 < total))(lambda: wait(ns))
                        row = jnp.where(ends, 0, (u0 + SUB) * 256)
                        slot = jnp.where(ends & (c + 1 < total), ns, s)
                    at = pl.ds(pl.multiple_of(row, 256), 256)
                    pltpu.matmul_push_rhs(wa[slot, at, :], 0, 0)
                    pltpu.matmul_push_rhs(wb[slot, at, :], 0, 1)
                    if u == 0:
                        pl.when(i == 0)(pop)
                return carry
            lax.fori_loop(0, chunks * (CH // SUB), trip, 0)

        def pop1(par, f):
            for r in range(R):
                a = pltpu.matmul_pop(accs[par][0][r])
                b = pltpu.matmul_pop(accs[par][1][r])
                h[f, sl(r), :] = (a / (1.0 + jnp.exp(-a)) * b).astype(jnp.bfloat16)

        def put(j, op):
            cols = pl.ds(pl.multiple_of(j * 512, 512), 512)

            def go(first, m):
                cp = pltpu.make_async_copy(ob.at[pl.ds(0, m), cols], o_ref.at[pl.ds(first, m), cols], so.at[j])
                getattr(cp, op)()
            pl.when(base == 0)(lambda: go(0, rows))
            pl.when(base > 0)(lambda: go(rows, t - rows))

        def pop2(par, j):
            c0 = pl.multiple_of(j * 512, 512)
            for r in range(big):
                first = pl.multiple_of((base if resident else 0) + r * RB, RB)
                if r < R:
                    a = pltpu.matmul_pop(accs[par][0][r]).astype(jnp.bfloat16)
                    b = pltpu.matmul_pop(accs[par][1][r]).astype(jnp.bfloat16)
                else:
                    a = b = z

                def store(first=first, a=a, b=b):
                    ob[pl.ds(first, RB), pl.ds(c0, 256)] = a
                    ob[pl.ds(first, RB), pl.ds(pl.multiple_of(c0 + 256, 256), 256)] = b
                if resident and R == small and rows + r * RB >= t:
                    pl.when(first < t)(store)
                else:
                    store()

        iota = lax.broadcasted_iota(jnp.int32, (RB, 256), 0)
        for k in range(ts):
            for r in range(R):
                hit = iota + (base + r * RB) == dest[0:1, k * 256:(k + 1) * 256]
                oh[k, sl(r), :] = jnp.where(hit, 1.0, 0.0).astype(jnp.bfloat16)

        def xpush(j, k):
            c0 = pl.multiple_of(j * 512, 512)
            pltpu.matmul_push_rhs(xs[k * 256:(k + 1) * 256, pl.ds(c0, 256)], 0, 0)
            pltpu.matmul_push_rhs(xs[k * 256:(k + 1) * 256, pl.ds(pl.multiple_of(c0 + 256, 256), 256)], 0, 1)

        def popx(par, j):
            for r in range(R):
                xg[2 * j, sl(r), :] = pltpu.matmul_pop(accs[par][0][r]).astype(jnp.bfloat16)
                xg[2 * j + 1, sl(r), :] = pltpu.matmul_pop(accs[par][1][r]).astype(jnp.bfloat16)

        if not resident:
            pl.when(base == 0)(lambda: xpiece(0).wait())
        xpush(0, 0)

        def gat(i, carry):
            for par in range(2):
                j = 2 * i + par
                for k in range(ts):
                    if k == ts - 1 and not resident:
                        pl.when((base == 0) & (j + 1 < nn))(lambda: xpiece(j + 1).wait())
                    accumulate(par, lambda r: oh[k, sl(r), :])
                    if k < ts - 1:
                        xpush(j, k + 1)
                    else:
                        xpush(lax.rem(j + 1, nn), 0)
                    if k == 0:
                        popx(1 - par, lax.rem(j + nn - 1, nn))
            return carry
        lax.fori_loop(0, nn // 2, gat, 0)
        wait(0)
        pltpu.matmul_acc_lhs(accs[0][0][0], z, load_staged_rhs=0)
        pltpu.matmul_acc_lhs(accs[0][1][0], z, load_staged_rhs=0)
        push(0, 0)
        popx(1, nn - 1)

        def stage1(i, carry):
            for par in range(2):
                f = 2 * i + par
                pop = functools.partial(pop1, 1 - par, lax.rem(f + kf - 1, kf))
                if R == small:
                    rolled(f * cpf, cpf, xg, par, False, pop)
                else:
                    for q in range(cpf):
                        block(f * cpf + q, q, xg, par, False, pop if q == 0 else None)
            return carry
        lax.fori_loop(0, kf // 2, stage1, 0)
        pop1(1, kf - 1)

        def stage2(i, carry):
            for par in range(2):
                j = 2 * i + par
                c0 = c1 + j * cpn
                jp = lax.rem(j + nn - 1, nn)

                pop = functools.partial(pop2, 1 - par, jp)
                if R == small:
                    rolled(c0, cpn, h, par, True, pop)
                else:
                    block(c0, 0, h, par, True, pop)
                if not resident:
                    if par == 0:
                        pl.when(i > 0)(lambda: put(jp, "start"))
                    else:
                        put(jp, "start")
                if R != small:
                    def inner(q, carry):
                        block(c0 + q, q, h, par, True, None)
                        return carry
                    lax.fori_loop(1, cpn, inner, 0)
            return carry
        lax.fori_loop(0, nn // 2, stage2, 0)
        pltpu.matmul_acc_lhs(accs[0][0][0], z, load_staged_rhs=0)
        pltpu.matmul_acc_lhs(accs[0][1][0], z, load_staged_rhs=0)
        pop2(1, nn - 1)
        if not resident:
            put(nn - 1, "start")
        pltpu.matmul_pop(accs[0][0][0])
        pltpu.matmul_pop(accs[0][1][0])
        if not resident:
            for j in range(nn):
                put(j, "wait")

    def scoped(*refs):
        it = iter(refs)
        accs = [[[next(it) for _ in range(big)] for _ in range(2)] for _ in range(2)]

        def tile(s, carry):
            base = s * rows
            more = n > base + rows
            lax.cond(n - base <= small * RB, lambda: run(accs, base, more, small), lambda: run(accs, base, more, big))
            return carry
        lax.fori_loop(0, jnp.maximum((n + rows - 1) // rows, 1), tile, 0)
        if resident:
            @pl.when(n <= rows)
            def _():
                o_ref[rows:, :] = jnp.zeros((t - rows, o_ref.shape[1]), o_ref.dtype)
        else:
            pl.when(n <= rows)(spare.wait)

    pl.run_scoped(scoped, *[pltpu.ACC(q)((RB, 256), jnp.float32) for _ in range(2) for q in range(2) for _ in range(big)])


def mlp(axis, idx, x, w1, w3, w2, resident, big=11, small=6):
    t, d = x.shape
    ff = w1.shape[1]
    rows = big * RB
    hbm, vmem = pl.BlockSpec(memory_space=pltpu.HBM), pl.BlockSpec(memory_space=pltpu.VMEM)
    io = vmem if resident else hbm
    return pl.pallas_call(
        functools.partial(mlp_kernel, axis, big, small, resident),
        out_shape=jax.ShapeDtypeStruct((t, d), jnp.bfloat16),
        in_specs=[vmem, io, hbm, hbm, hbm],
        out_specs=io,
        scratch_shapes=[
            pltpu.VMEM((t // 256, rows, 256), jnp.bfloat16),
            pltpu.VMEM((d // 256, rows, 256), jnp.bfloat16),
            pltpu.VMEM((ff // 256, rows, 256), jnp.bfloat16),
            pltpu.VMEM((NS, CH * 256, 256), jnp.bfloat16),
            pltpu.VMEM((NS, CH * 256, 256), jnp.bfloat16),
            pltpu.SemaphoreType.DMA((NS,)),
            pltpu.SemaphoreType.DMA((NS,)),
        ]
        + ([] if resident else [
            pltpu.VMEM((t, d), jnp.bfloat16),
            pltpu.VMEM((rows, d), jnp.bfloat16),
            pltpu.VMEM((t - rows, d), jnp.bfloat16),
            pltpu.SemaphoreType.DMA((d // 512,)),
            pltpu.SemaphoreType.DMA((d // 512,)),
            pltpu.SemaphoreType.DMA,
        ]),
        compiler_params=pltpu.CompilerParams(vmem_limit_bytes=41 * 1024 * 1024),
        cost_estimate=pl.CostEstimate(flops=6 * rows * d * ff, bytes_accessed=6 * d * ff, transcendentals=0),
        name="expert_rows",
    )(idx, x, w1, w3, w2)


def prep_kernel(axis, n, x_ref, wr_ref, idx_ref, g_ref, d_ref):
    t = x_ref.shape[0]
    me = lax.axis_index(axis)
    logits = jnp.dot(x_ref[...], wr_ref[...], preferred_element_type=jnp.float32)
    i0, i1 = idx_ref[:, 0:1], idx_ref[:, 1:2]
    s0 = jnp.zeros((t, 1), jnp.float32)
    s1 = jnp.zeros((t, 1), jnp.float32)
    for e in range(n):
        s0 = s0 + jnp.where(i0 == e, logits[:, e:e + 1], 0.0)
        s1 = s1 + jnp.where(i1 == e, logits[:, e:e + 1], 0.0)
    m = jnp.maximum(s0, s1)
    p0, p1 = jnp.exp(s0 - m), jnp.exp(s1 - m)
    g0, g1 = p0 / (p0 + p1), p1 / (p0 + p1)
    slot = lax.broadcasted_iota(jnp.int32, (1, n), 1)
    e = me ^ slot
    h0, h1 = jnp.where(i0 == e, 1.0, 0.0), jnp.where(i1 == e, 1.0, 0.0)
    g_ref[...] = h0 * g0 + h1 * g1
    has = h0 + h1
    tri = lax.broadcasted_iota(jnp.int32, (t, t), 0) >= lax.broadcasted_iota(jnp.int32, (t, t), 1)
    tri = jnp.where(tri, 1.0, 0.0).astype(jnp.bfloat16)
    cnt = jnp.dot(tri, has.astype(jnp.bfloat16), preferred_element_type=jnp.float32)
    d_ref[...] = jnp.where(has > 0.0, cnt.astype(jnp.int32) - 1, -1)


def prep(axis, n, x, wr, idx):
    t, d = x.shape
    vm = pl.BlockSpec(memory_space=pltpu.VMEM)
    return pl.pallas_call(
        functools.partial(prep_kernel, axis, n),
        out_shape=(jax.ShapeDtypeStruct((t, n), jnp.float32), jax.ShapeDtypeStruct((t, n), jnp.int32)),
        in_specs=[vm] * 3,
        out_specs=(vm,) * 2,
        cost_estimate=pl.CostEstimate(flops=2 * t * d * 128, bytes_accessed=t * d * 2, transcendentals=0),
        compiler_params=pltpu.CompilerParams(vmem_limit_bytes=12 * 1024 * 1024),
        name="gates",
    )(x, wr, idx)


def combine_kernel(d_ref, g_ref, o0, o3, h1, h2, y_ref, sel, gb, ya, yt, b1, b2, s1, s2, sy):
    t, width = y_ref.shape
    nn = width // 512
    nr = t // RB
    ts = t // 256

    def cols(j):
        return pl.ds(pl.multiple_of(j * 512, 512), 512)

    def load(j, i):
        h, b, s = ((h1, b1, s1), (h2, b2, s2))[i]
        return pltpu.make_async_copy(h.at[:, cols(j)], b.at[:, cols(j)], s.at[j])

    def out(j):
        return pltpu.make_async_copy(yt.at[lax.rem(j, 2)], y_ref.at[:, cols(j)], sy.at[lax.rem(j, 2)])

    for j in range(nn):
        load(j, 0).start()
        load(j, 1).start()
    order = ((0, o0), (3, o3), (1, b1), (2, b2))
    iota = lax.broadcasted_iota(jnp.int32, (t, t), 1)
    for e in range(len(order)):
        sel[e] = jnp.where(iota == d_ref[:, e:e + 1], 1.0, 0.0).astype(jnp.bfloat16)
        gb[e] = jnp.broadcast_to(g_ref[:, e:e + 1], gb.shape[1:])

    def sl(r):
        return slice(r * RB, (r + 1) * RB)

    def push(o, j, k):
        c0 = pl.multiple_of(j * 512, 512)
        pltpu.matmul_push_rhs(o[k * 256:(k + 1) * 256, pl.ds(c0, 256)], 0, 0)
        pltpu.matmul_push_rhs(o[k * 256:(k + 1) * 256, pl.ds(pl.multiple_of(c0 + 256, 256), 256)], 0, 1)

    def scoped(*refs):
        it = iter(refs)
        accs = [[[next(it) for _ in range(nr)] for _ in range(2)] for _ in range(2)]

        def drain(par, i, slot):
            e = order[i][0]
            for r in range(nr):
                g = gb[e, sl(r), :]
                for q in range(2):
                    p = pltpu.matmul_pop(accs[par][q][r])
                    for c in range(2):
                        at = slice(q * 256 + c * 128, q * 256 + (c + 1) * 128)
                        v = g * p[:, c * 128:(c + 1) * 128]
                        if i > 0:
                            v = ya[sl(r), at] + v
                        if i < len(order) - 1:
                            ya[sl(r), at] = v
                        else:
                            yt[slot, sl(r), at] = v.astype(yt.dtype)

        push(o0, 0, 0)

        def step(j, carry):
            slot = lax.rem(j + 1, 2)
            for i, (e, o) in enumerate(order):
                for k in range(ts):
                    for r in range(nr):
                        v = sel[e, sl(r), k * 256:(k + 1) * 256]
                        for q in range(2):
                            pltpu.matmul_acc_lhs(accs[i % 2][q][r], v, load_staged_rhs=0 if r == 0 else None)
                    if k + 1 < ts:
                        push(o, j, k + 1)
                    elif i + 1 < len(order):
                        if i + 1 >= 2:
                            load(j, i - 1).wait()
                        push(order[i + 1][1], j, 0)
                    else:
                        push(o0, lax.rem(j + 1, nn), 0)
                    if k == 0:
                        if i == 0:
                            pl.when(j > 2)(lambda: out(j - 3).wait())
                            drain(1, len(order) - 1, slot)
                            pl.when(j > 0)(lambda: out(j - 1).start())
                        else:
                            drain((i - 1) % 2, i - 1, slot)
            return carry
        lax.fori_loop(0, nn, step, 0)
        z = jnp.zeros((RB, 256), jnp.bfloat16)
        for q in range(2):
            pltpu.matmul_acc_lhs(accs[0][q][0], z, load_staged_rhs=0)
        out(nn - 3).wait()
        drain(1, len(order) - 1, (nn - 1) % 2)
        out(nn - 1).start()
        for q in range(2):
            pltpu.matmul_pop(accs[0][q][0])
        out(nn - 2).wait()
        out(nn - 1).wait()

    pl.run_scoped(scoped, *[pltpu.ACC(q)((RB, 256), jnp.float32) for _ in range(2) for q in range(2) for _ in range(nr)])


def combine(d, g, outs):
    t, width = outs[0].shape
    k = len(outs)
    hbm, vmem = pl.BlockSpec(memory_space=pltpu.HBM), pl.BlockSpec(memory_space=pltpu.VMEM)
    return pl.pallas_call(
        combine_kernel,
        out_shape=jax.ShapeDtypeStruct((t, width), jnp.bfloat16),
        in_specs=[vmem] * 4 + [hbm] * 2,
        out_specs=hbm,
        scratch_shapes=[
            pltpu.VMEM((k, t, t), jnp.bfloat16),
            pltpu.VMEM((k, t, 128), jnp.float32),
            pltpu.VMEM((t, 512), jnp.float32),
            pltpu.VMEM((2, t, 512), jnp.bfloat16),
            pltpu.VMEM((t, width), jnp.bfloat16),
            pltpu.VMEM((t, width), jnp.bfloat16),
            pltpu.SemaphoreType.DMA((width // 512,)),
            pltpu.SemaphoreType.DMA((width // 512,)),
            pltpu.SemaphoreType.DMA((2,)),
        ],
        compiler_params=pltpu.CompilerParams(vmem_limit_bytes=28 * 1024 * 1024),
        cost_estimate=pl.CostEstimate(flops=2 * k * t * t * width, bytes_accessed=(k + 1) * t * width * 2, transcendentals=0),
        name="combine_rows",
    )(d, g, outs[0], outs[3], outs[1], outs[2])


def solution(mesh):
    n = mesh.shape['expert']

    def hop(a, bit):
        return lax.ppermute(a, 'expert', [(i, i ^ bit) for i in range(n)])

    def local(x, idx, wr, w1, w3, w2):
        w1, w3, w2 = w1[0], w3[0], w2[0]
        idx_1, x_1 = hop(idx, 1), hop(x, 1)
        idx_2, x_2 = hop(idx, 2), hop(x, 2)
        idx_3, x_3 = hop(idx_2, 1), hop(x_2, 1)
        g, d = prep('expert', n, x, wr, idx)
        outs, tie = {}, None
        for b, (xi, ii) in {1: (x_1, idx_1), 2: (x_2, idx_2), 3: (x_3, idx_3), 0: (x, idx)}.items():
            if tie is not None:
                ii, outs[tie] = lax.optimization_barrier((ii, outs[tie]))
            outs[b] = mlp('expert', ii.T, xi, w1, w3, w2, resident=b in (3, 0))
            tie = b
        back = [outs[0]] + [hop(outs[b], b) for b in (1, 2, 3)]
        return combine(d, g, back)

    tok = P(('data', 'expert'), None)
    wsp = P('expert', None, None)
    return jax.shard_map(local, mesh=mesh, in_specs=(tok, tok, P(), wsp, wsp, wsp), out_specs=tok, check_vma=False)
```
